32 devices in a mesh: pb: 2 (over x), ka: 16 (over z, y, core).
Axes of the slice: x: 2, y: 2, z: 4, core: 2. Of those that a mesh axis runs over, the one named last changes fastest.
Arguments:
- coupling: bfloat16 [2, 16, 32, 32, 384], P('pb', 'ka'), may hold values from -0.796875 to 0.796875
- phonon_occ: float32 [2, 16, 32, 12], P('pb', 'ka'), may hold values from 0.1 to 1
- band_window: int32 [2, 16, 32, 32], P('pb', 'ka'), may hold values 0 or 1
- pair_count: int32 [2, 16, 16], P('pb', 'ka'), may hold values from 0 to 2, as said below
- k_target: int32 [2, 16, 32], P('pb', 'ka'), may hold values from 0 to 127
- kq_source: int32 [2, 16, 32], P('pb', 'ka'), may hold values from 0 to 127
- velocity: float32 [3, 32, 2048], P(None, None, 'ka'), may hold values from -6 to 6
- lifetime: float32 [32, 2048], P(None, 'ka'), may hold values from 0.5 to 2
Outputs:
- deviation: float32 [3, 32, 2048], P(None, None, 'ka')
The draws below stay inside these ranges and needn't reach their ends.
Inputs may be any that keep to these rules, and one draw needn't show every extreme that they name: pair_count[p, a, d] is the number of live tile slots among slots d * 2 to d * 2 + 1 of device (p, a); in every q-group p some owner d receives 2 live tiles from every source.
All inputs are finite; a program needn't handle non-finite values. No bound on the sum of `band_window` on one device may be relied on, other than what follows from the above.
Results may differ from the reference program's by a relative error of at most 0.012.
Values may be sent and summed in bfloat16 or wider, within the bound.
A program may use at most 64 MiB of HBM per device.

```python
import math
import jax
import jax.numpy as jnp
from jax import lax

BANDS = 32
MODES = 12
K_DEV = 128
TILE_SLOTS = 2
ITERS = 4
KPOINTS = 2048
TILES = 32
N_PB = 2
N_KA = 16


def draw_pair_count(key, part):
    first_key, second_key = jax.random.split(jax.random.fold_in(key, 17), 2)
    base = jax.random.randint(first_key, (N_PB, N_KA, N_KA), 0, TILE_SLOTS + 1)
    busiest = jax.random.randint(second_key, (N_PB, 1, 1), 0, N_KA)
    column = jnp.arange(N_KA)[None, None, :] == busiest
    return jnp.where(column, TILE_SLOTS, base).astype(jnp.int32)


def set_ends(drawn, rng, least, high):
    index_at = [jax.random.randint(jax.random.fold_in(rng, axis), (), 0, length) for axis, length in enumerate(drawn.shape)]
    main_axis = drawn.shape.index(max(drawn.shape))
    neighbour = index_at[:main_axis] + [(index_at[main_axis] + 1) % drawn.shape[main_axis]] + index_at[main_axis + 1:]
    return drawn.at[tuple(index_at)].set(least).at[tuple(neighbour)].set(high)


def levels(own_key, shape, cuts, low, top_value):
    level, own = 1.0, jax.random.fold_in(own_key, 6)
    for position, blocks in cuts:
        heights = jnp.exp(jax.random.uniform(jax.random.fold_in(own, position), (blocks,), jnp.float32, low / len(cuts), top_value / len(cuts)))
        level = level * jnp.repeat(heights, shape[position] // blocks).reshape([-1 if axis == position else 1 for axis in range(len(shape))])
    return level


def gaussian(own_key, shape, spread, bound, pieces=(), held_as=jnp.bfloat16):
    array = spread * jax.random.normal(own_key, shape, jnp.float32)
    if pieces:
        array = array * levels(own_key, shape, pieces, -0.22, 0.18)
    return jnp.clip(array, -bound, bound).astype(held_as)


def setup_inputs(seed: int = 0) -> dict:
    seeds = jax.random.split(jax.random.key(seed), 9)
    return {
        "coupling": gaussian(seeds[0], (N_PB, N_KA, TILES, BANDS, BANDS * MODES), 0.1, 0.796875, ((0, 2), (1, 16))),
        "phonon_occ": jnp.clip(jnp.exp(math.log(1.0) - 2.3025851 * jax.random.uniform(seeds[1], (N_PB, N_KA, TILES, MODES), jnp.float32) ** levels(seeds[1], (N_PB, N_KA, TILES, MODES), ((0, 2), (1, 16)), -0.2, 0.2)), 0.1, 1.0),
        "band_window": set_ends((jax.random.randint(seeds[2], (N_PB, N_KA, TILES, BANDS), 0, 4) < 3).astype(jnp.int32), jax.random.fold_in(seeds[2], 1), 0, 1),
        "pair_count": draw_pair_count(jax.random.fold_in(seeds[8], 71), 0),
        "k_target": set_ends(jax.random.randint(seeds[4], (N_PB, N_KA, TILES), 0, K_DEV), jax.random.fold_in(seeds[4], 1), 0, K_DEV - 1).astype(jnp.int32),
        "kq_source": set_ends(jax.random.randint(seeds[5], (N_PB, N_KA, TILES), 0, K_DEV), jax.random.fold_in(seeds[5], 1), 0, K_DEV - 1).astype(jnp.int32),
        "velocity": gaussian(seeds[6], (3, BANDS, KPOINTS), 1.0, 6.0, ((2, 16),), jnp.float32),
        "lifetime": jnp.clip(jnp.exp(math.log(2.0) - 1.3862944 * jax.random.uniform(seeds[7], (BANDS, KPOINTS), jnp.float32) ** levels(seeds[7], (BANDS, KPOINTS), ((1, 16),), -0.2, 0.2)), 0.5, 2.0),
    }


def weigh_tile(coupling_tile, occ_tile, slot_live, window):
    squared = coupling_tile.astype(jnp.float32) * coupling_tile.astype(jnp.float32)
    squared = squared.reshape(squared.shape[0], BANDS, BANDS, MODES)
    summed = jnp.sum(squared * occ_tile[:, None, None, :], axis=3)
    masked = slot_live[:, None] * window
    return (summed * masked[:, :, None]).astype(jnp.bfloat16)


def reference(coupling, phonon_occ, band_window, pair_count, k_target, kq_source, velocity, lifetime):
    tile_count = N_KA * TILE_SLOTS
    block_count = N_PB * N_KA
    slot_live = (jnp.arange(TILE_SLOTS)[None, None, None, :] < pair_count[:, :, :, None])
    slot_live = slot_live.reshape(block_count, tile_count).astype(jnp.float32)
    coupling_blocks = coupling.reshape(block_count, tile_count, BANDS, BANDS * MODES)
    occ_blocks = phonon_occ.reshape(block_count, tile_count, MODES)
    window_blocks = band_window.reshape(block_count, tile_count, BANDS).astype(jnp.float32)
    target_blocks = k_target.reshape(block_count, tile_count)
    source_blocks = kq_source.reshape(block_count, tile_count)
    block_owner = (jnp.arange(block_count) % N_KA).astype(jnp.int32)
    owner = (jnp.arange(tile_count) // TILE_SLOTS).astype(jnp.int32)
    deviation = lifetime[None] * velocity
    for iteration in range(ITERS):
        rounded = deviation.astype(jnp.bfloat16)

        def block_term(scatter_total, items):
            coupling_tile, occ_tile, live_tile, window, target, source_local, source_block = items
            weight = weigh_tile(coupling_tile, occ_tile, live_tile, window)
            columns = (source_block * K_DEV + source_local).astype(jnp.int32)
            chosen = jnp.take(rounded, columns, axis=2)
            contribution = jnp.einsum("tnm,dmt->dnt", weight.astype(jnp.float32), chosen.astype(jnp.float32), precision=lax.Precision.HIGHEST)
            global_k = (owner * K_DEV + target).astype(jnp.int32)
            return scatter_total.at[:, :, global_k].add(contribution), None

        start_total = jnp.zeros((3, BANDS, K_DEV * N_KA), jnp.float32)
        scattering, unused = lax.scan(block_term, start_total, (coupling_blocks, occ_blocks, slot_live, window_blocks, target_blocks, source_blocks, block_owner))
        deviation = lifetime[None] * (velocity + scattering)
    return deviation
```

```python
import functools

import jax
import jax.numpy as jnp
from jax import lax
from jax.experimental import pallas as pl
from jax.experimental.pallas import tpu as pltpu
from jax.sharding import PartitionSpec as P

ITERS = 4
LANES = 128
F32 = jnp.float32
BF16 = jnp.bfloat16


def iota(shape, axis):
    return lax.broadcasted_iota(jnp.int32, shape, axis)


def mask(condition):
    return jnp.where(condition, 1.0, 0.0)


def dot(a, b, dims=((1,), (0,)), precision=None):
    return lax.dot_general(a, b, (dims, ((), ())), precision=precision, preferred_element_type=F32)


def column(row, wanted):
    rows, width = wanted.shape
    return jnp.sum(jnp.where(wanted, jnp.broadcast_to(row, (rows, width)), 0.0), axis=1, keepdims=True)


def kernel(
    n_pb, n_ka, directions,
    coupling_hbm, occ_ref, window_ref, count_ref, target_ref, source_ref, velocity_ref, lifetime_ref,
    out_ref,
    coupling_ref, send, recv, load_sem, send_sem, recv_sem,
):
    p, a = lax.axis_index("pb"), lax.axis_index("ka")
    me = p * n_ka + a
    devices = n_pb * n_ka
    tiles, bands = window_ref.shape
    slots = tiles // n_ka
    modes = occ_ref.shape[1]
    wide = bands * modes
    width = velocity_ref.shape[1]
    row = recv.shape[-1]
    used = directions * bands
    low = 256 // bands
    span = low * bands
    groups = tiles // low

    load = pltpu.make_async_copy(coupling_hbm, coupling_ref, load_sem)
    load.start()
    barrier = pltpu.get_barrier_semaphore()

    def peer(step):
        other = lax.rem(me + step, devices)
        return {"pb": other // n_ka, "ka": lax.rem(other, n_ka)}

    def greet(step, carry):
        pl.semaphore_signal(barrier, inc=1, device_id=peer(step), device_id_type=pl.DeviceIdType.MESH)
        return carry

    lax.fori_loop(1, devices, greet, 0)

    eye = iota((tiles, tiles), 0) == iota((tiles, tiles), 1)
    owner = iota((tiles, n_ka), 0) // slots == iota((tiles, n_ka), 1)
    live = mask((iota((tiles, 1), 0) % slots).astype(F32) < column(count_ref[...].astype(F32), owner))
    source = column(source_ref[...].astype(F32), eye)
    target = column(target_ref[...].astype(F32), eye)
    pick = mask(source == iota((tiles, width), 1).astype(F32)).astype(BF16)
    target_lane = jnp.where(iota((tiles, row), 1) == used, target, 0.0)
    shown = window_ref[...].astype(F32) * live
    keep = jnp.concatenate([shown] * groups, axis=1)
    keep = jnp.where(iota((tiles, groups * bands), 1) // bands == iota((tiles, groups * bands), 0) // low, keep, 0.0)
    keep = jnp.concatenate([keep] * directions, axis=0)
    place = mask(
        (iota((tiles, directions * span), 1) % span) // bands == iota((tiles, directions * span), 0) % low
    )
    shape = (row, directions * span)
    spread = mask(
        ((iota(shape, 0) // bands) == (iota(shape, 1) // span)) & (iota(shape, 0) % bands == iota(shape, 1) % bands)
    ).astype(BF16)
    shape = (directions * groups * bands, row)
    fold = mask(
        ((iota(shape, 0) // (groups * bands)) == (iota(shape, 1) // bands))
        & (iota(shape, 0) % bands == iota(shape, 1) % bands)
    ).astype(BF16)

    pad = jnp.zeros((row - used, width), F32)
    velocity = jnp.concatenate([velocity_ref[...], pad], axis=0).T
    lifetime = jnp.concatenate([lifetime_ref[...]] * directions + [pad], axis=0).T

    shape = (modes, wide)
    occ = dot(occ_ref[...], mask(iota(shape, 1) % modes == iota(shape, 0)), precision=lax.Precision.HIGHEST)
    shape = (wide, LANES)
    start = (iota(shape, 1) % bands) * modes
    gather = mask((iota(shape, 0) >= start) & (iota(shape, 0) < start + modes)).astype(BF16)
    per = LANES // bands
    lane_block = iota((bands, LANES), 1) // bands
    load.wait()
    weight = []
    for group in range(groups):
        halves = []
        for half in range(low // per):
            total = jnp.zeros((bands, LANES), F32)
            for inner in range(per):
                tile = group * low + half * per + inner
                value = coupling_ref[tile].astype(F32)
                value = (value * value * occ[tile : tile + 1, :]).astype(BF16)
                total = jnp.where(lane_block == inner, dot(value, gather), total)
            halves.append(total)
        weight.append(jnp.concatenate(halves, axis=1))
    weight = jnp.concatenate(weight, axis=0).astype(BF16)

    deviation = lifetime * velocity
    scatter = None
    for step in range(ITERS):
        chosen = dot(pick, deviation.astype(BF16)).astype(BF16)
        chosen = (dot(chosen, spread) * place).astype(BF16)
        chosen = jnp.concatenate([chosen[:, i * span : (i + 1) * span] for i in range(directions)], axis=0)
        terms = (dot(chosen, weight, ((1,), (1,))) * keep).astype(BF16)
        terms = jnp.concatenate([terms[i * tiles : (i + 1) * tiles] for i in range(directions)], axis=1)
        terms = (dot(terms, fold) + target_lane).astype(BF16)
        send[step] = terms.reshape(n_ka, slots, row)
        if step == 0:
            pl.semaphore_wait(barrier, devices - 1)

        def post(distance, carry):
            other = lax.rem(me + distance, devices)
            pltpu.make_async_remote_copy(
                src_ref=send.at[step, lax.rem(other, n_ka)],
                dst_ref=recv.at[step, me],
                send_sem=send_sem.at[step],
                recv_sem=recv_sem.at[step],
                device_id=peer(distance),
                device_id_type=pl.DeviceIdType.MESH,
            ).start()
            return carry

        pltpu.make_async_copy(send.at[step, a], recv.at[step, me], recv_sem.at[step]).start()
        lax.fori_loop(1, devices, post, 0)
        pltpu.make_async_copy(recv.at[step], recv.at[step], recv_sem.at[step]).wait()
        arrived = recv[step].reshape(devices * slots, row)
        if scatter is None:
            shape = (devices * slots, width)
            scatter = mask(arrived[:, used : used + 1].astype(F32) == iota(shape, 1).astype(F32)).T.astype(BF16)
        deviation = lifetime * (velocity + dot(scatter, arrived))
    out_ref[...] = deviation.T[:used]
    for step in range(ITERS):
        sent = recv.at[step, pl.ds(0, devices - 1)]
        pltpu.make_async_copy(sent, sent, send_sem.at[step]).wait()


def shards(n_pb, n_ka, coupling, phonon_occ, band_window, pair_count, k_target, kq_source, velocity, lifetime):
    tiles = coupling.shape[2]
    directions, bands, width = velocity.shape
    slots = tiles // n_ka
    row = -(-(directions * bands + 1) // LANES) * LANES
    vmem = pl.BlockSpec(memory_space=pltpu.VMEM)
    out = pl.pallas_call(
        functools.partial(kernel, n_pb, n_ka, directions),
        out_shape=jax.ShapeDtypeStruct((directions * bands, width), F32),
        in_specs=[pl.BlockSpec(memory_space=pl.ANY)] + [vmem] * 7,
        out_specs=vmem,
        scratch_shapes=[
            pltpu.VMEM(coupling.shape[2:], coupling.dtype),
            pltpu.VMEM((ITERS, n_ka, slots, row), BF16),
            pltpu.VMEM((ITERS, n_pb * n_ka, slots, row), BF16),
            pltpu.SemaphoreType.DMA,
            pltpu.SemaphoreType.DMA((ITERS,)),
            pltpu.SemaphoreType.DMA((ITERS,)),
        ],
        compiler_params=pltpu.CompilerParams(collective_id=0, has_side_effects=True),
    )(
        coupling[0, 0], phonon_occ[0, 0], band_window[0, 0], pair_count[0], k_target[0], kq_source[0],
        velocity.reshape(directions * bands, width), lifetime,
    )
    return out.reshape(directions, bands, width)


def solution(mesh):
    placed = (
        P("pb", "ka", None, None, None),
        P("pb", "ka", None, None),
        P("pb", "ka", None, None),
        P("pb", "ka", None),
        P("pb", "ka", None),
        P("pb", "ka", None),
        P(None, None, "ka"),
        P(None, "ka"),
    )
    return jax.shard_map(
        functools.partial(shards, mesh.shape["pb"], mesh.shape["ka"]),
        mesh=mesh, in_specs=placed, out_specs=P(None, None, "ka"), check_vma=False,
    )
```

```python
import functools

import jax
import jax.numpy as jnp
from jax import lax
from jax.experimental import pallas as pl
from jax.experimental.pallas import tpu as pltpu
from jax.sharding import PartitionSpec as P

ITERS = 4
LANES = 128
UNROLLED = 16
F32 = jnp.float32
BF16 = jnp.bfloat16


def iota(shape, axis):
    return lax.broadcasted_iota(jnp.int32, shape, axis)


def mask(condition):
    return jnp.where(condition, 1.0, 0.0)


def dot(a, b, dims=((1,), (0,)), precision=None):
    return lax.dot_general(a, b, (dims, ((), ())), precision=precision, preferred_element_type=F32)


def column(row, wanted):
    rows, width = wanted.shape
    return jnp.sum(jnp.where(wanted, jnp.broadcast_to(row, (rows, width)), 0.0), axis=1, keepdims=True)


def each(count, act):
    if count <= 2 * UNROLLED:
        for distance in sorted(range(1, count), key=lambda d: -min(d, count - d)):
            act(distance)
    else:

        def body(distance, carry):
            act(distance)
            return carry

        lax.fori_loop(1, count, body, 0)


def kernel(
    n_pb, n_ka, directions,
    coupling_hbm, occ_ref, window_ref, count_ref, target_ref, source_ref, velocity_ref, lifetime_ref,
    out_ref,
    coupling_ref, weights, tables, send, recv, load_sem, send_sem, recv_sem, share_send, share_recv,
):
    p, a = lax.axis_index("pb"), lax.axis_index("ka")
    me = p * n_ka + a
    devices = n_pb * n_ka
    tiles, bands = window_ref.shape
    slots = tiles // n_ka
    modes = occ_ref.shape[0]
    wide = bands * modes
    width = velocity_ref.shape[1]
    row = recv.shape[-1]
    used = directions * bands
    low = 256 // bands
    span = low * bands
    groups = tiles // low

    load = pltpu.make_async_copy(coupling_hbm, coupling_ref, load_sem)
    load.start()
    barrier = pltpu.get_barrier_semaphore()

    def peer(step):
        other = lax.rem(me + step, devices)
        return {"pb": other // n_ka, "ka": lax.rem(other, n_ka)}

    def greet(distance):
        pl.semaphore_signal(barrier, inc=1, device_id=peer(distance), device_id_type=pl.DeviceIdType.MESH)

    each(devices, greet)

    eye = iota((tiles, tiles), 0) == iota((tiles, tiles), 1)
    owner = iota((tiles, n_ka), 0) // slots == iota((tiles, n_ka), 1)
    live = mask((iota((tiles, 1), 0) % slots).astype(F32) < column(count_ref[...].astype(F32), owner))
    source = column(source_ref[...].astype(F32), eye)
    target = column(target_ref[...].astype(F32), eye)
    target_lane = jnp.where(iota((tiles, row), 1) == used, target, 0.0)
    shown = window_ref[...].astype(F32) * live

    def tile_tables(shown, source):
        pick = mask(source == iota((tiles, width), 1).astype(F32)).astype(BF16)
        keep = jnp.concatenate([shown] * groups, axis=1)
        at = (tiles, groups * bands)
        keep = jnp.where(iota(at, 1) // bands == iota(at, 0) // low, keep, 0.0)
        return pick, jnp.concatenate([keep] * directions, axis=0)

    own = tile_tables(shown, source)
    tables[p] = jnp.concatenate(
        [shown, jnp.where(iota((tiles, LANES - bands), 1) == 0, source, 0.0)], axis=1
    ).astype(BF16)
    place = mask(
        (iota((tiles, directions * span), 1) % span) // bands == iota((tiles, directions * span), 0) % low
    )
    shape = (row, directions * span)
    spread = mask(
        ((iota(shape, 0) // bands) == (iota(shape, 1) // span)) & (iota(shape, 0) % bands == iota(shape, 1) % bands)
    ).astype(BF16)
    shape = (directions * groups * bands, row)
    fold = mask(
        ((iota(shape, 0) // (groups * bands)) == (iota(shape, 1) // bands))
        & (iota(shape, 0) % bands == iota(shape, 1) % bands)
    ).astype(BF16)

    pad = jnp.zeros((row - used, width), F32)
    velocity = jnp.concatenate([velocity_ref[...], pad], axis=0).T
    lifetime = jnp.concatenate([lifetime_ref[...]] * directions + [pad], axis=0).T

    shape = (modes, wide)
    occ = dot(
        occ_ref[:, 0, :], mask(iota(shape, 1) % modes == iota(shape, 0)), ((0,), (0,)), lax.Precision.HIGHEST
    )
    shape = (wide, LANES)
    start = (iota(shape, 1) % bands) * modes
    gather = mask((iota(shape, 0) >= start) & (iota(shape, 0) < start + modes)).astype(BF16)
    per = LANES // bands
    lane_block = iota((bands, LANES), 1) // bands
    load.wait()
    weight = []
    for group in range(groups):
        halves = []
        for half in range(low // per):
            total = jnp.zeros((bands, LANES), F32)
            for inner in range(per):
                tile = group * low + half * per + inner
                value = coupling_ref[tile].astype(F32)
                value = (value * value * occ[tile : tile + 1, :]).astype(BF16)
                total = jnp.where(lane_block == inner, dot(value, gather), total)
            halves.append(total)
        weight.append(jnp.concatenate(halves, axis=1))
    weight = jnp.concatenate(weight, axis=0).astype(BF16)
    weights[p] = weight

    def share(distance, held, index):
        return pltpu.make_async_remote_copy(
            src_ref=held.at[p],
            dst_ref=held.at[p],
            send_sem=share_send.at[index],
            recv_sem=share_recv.at[index],
            device_id={"pb": lax.rem(p + distance, n_pb), "ka": a},
            device_id_type=pl.DeviceIdType.MESH,
        )

    def tile_terms(chosen, pick_keep_weight):
        keep, weight = pick_keep_weight
        chosen = (dot(chosen, spread) * place).astype(BF16)
        chosen = jnp.concatenate([chosen[:, i * span : (i + 1) * span] for i in range(directions)], axis=0)
        terms = (dot(chosen, weight, ((1,), (1,))) * keep).astype(BF16)
        terms = jnp.concatenate([terms[i * tiles : (i + 1) * tiles] for i in range(directions)], axis=1)
        return dot(terms, fold)

    deviation = lifetime * velocity

    terms = tile_terms(dot(own[0], deviation.astype(BF16)).astype(BF16), (own[1], weight)) + target_lane
    send[0, 0] = terms.astype(BF16).reshape(n_ka, slots, row)
    pl.semaphore_wait(barrier, devices - 1)

    def post_all(distance):
        to = peer(distance)
        pltpu.make_async_remote_copy(
            src_ref=send.at[0, 0, to["ka"]],
            dst_ref=recv.at[0, p, a],
            send_sem=send_sem.at[0],
            recv_sem=recv_sem.at[0],
            device_id=to,
            device_id_type=pl.DeviceIdType.MESH,
        ).start()

    each(devices, post_all)
    pltpu.make_async_copy(send.at[0, 0, a], recv.at[0, p, a], recv_sem.at[0]).start()
    for distance in range(1, n_pb):
        share(distance, tables, 0).start()
        share(distance, weights, 1).start()
    for index, held in enumerate((tables, weights)):
        part = held.at[pl.ds(0, n_pb - 1)]
        pltpu.make_async_copy(part, part, share_recv.at[index]).wait()
    picks, keeps = [], []
    for q in range(n_pb):
        table = tables[q].astype(F32)
        pick, keep = tile_tables(table[:, :bands], table[:, bands : bands + 1])
        picks.append(pick)
        keeps.append(keep)
    pick = jnp.concatenate(picks, axis=0)

    def receive(step):
        pltpu.make_async_copy(recv.at[step], recv.at[step], recv_sem.at[step]).wait()
        return recv[step].reshape(devices * slots, row)

    arrived = receive(0)
    shape = (devices * slots, width)
    scatter = mask(arrived[:, used : used + 1].astype(F32) == iota(shape, 1).astype(F32)).T.astype(BF16)
    deviation = lifetime * (velocity + dot(scatter, arrived))

    for step in range(1, ITERS):
        chosen = dot(pick, deviation.astype(BF16)).astype(BF16)
        for q in range(n_pb):
            terms = tile_terms(chosen[q * tiles : (q + 1) * tiles], (keeps[q], weights[q]))
            send[step, q] = terms.astype(BF16).reshape(n_ka, slots, row)

        def post(distance):
            other = lax.rem(a + distance, n_ka)
            pltpu.make_async_remote_copy(
                src_ref=send.at[step, :, other],
                dst_ref=recv.at[step, :, a],
                send_sem=send_sem.at[step],
                recv_sem=recv_sem.at[step],
                device_id={"pb": p, "ka": other},
                device_id_type=pl.DeviceIdType.MESH,
            ).start()

        each(n_ka, post)
        pltpu.make_async_copy(send.at[step, :, a], recv.at[step, :, a], recv_sem.at[step]).start()
        deviation = lifetime * (velocity + dot(scatter, receive(step)))
    out_ref[...] = deviation.T[:used]
    for step in range(ITERS):
        if step:
            pieces = [recv.at[step, :, pl.ds(0, n_ka - 1)]]
        else:
            pieces = [recv.at[0, pl.ds(0, n_pb - 1)]] if n_pb > 1 else []
            pieces = pieces + [recv.at[0, 0, pl.ds(0, n_ka - 1)]]
        for piece in pieces:
            pltpu.make_async_copy(piece, piece, send_sem.at[step]).wait()
    for index, held in enumerate((tables, weights)):
        part = held.at[pl.ds(0, n_pb - 1)]
        pltpu.make_async_copy(part, part, share_send.at[index]).wait()


def shards(n_pb, n_ka, coupling, phonon_occ, band_window, pair_count, k_target, kq_source, velocity, lifetime):
    tiles = coupling.shape[2]
    directions, bands, width = velocity.shape
    slots = tiles // n_ka
    low = 256 // bands
    row = -(-(directions * bands + 1) // LANES) * LANES
    vmem = pl.BlockSpec(memory_space=pltpu.VMEM)
    out = pl.pallas_call(
        functools.partial(kernel, n_pb, n_ka, directions),
        out_shape=pltpu.VMEM((directions * bands, width), F32),
        in_specs=[pl.BlockSpec(memory_space=pl.ANY)] + [vmem] * 7,
        out_specs=vmem,
        scratch_shapes=[
            pltpu.VMEM(coupling.shape[2:], coupling.dtype),
            pltpu.VMEM((n_pb, tiles // low * bands, low * bands), BF16),
            pltpu.VMEM((n_pb, tiles, LANES), BF16),
            pltpu.VMEM((ITERS, n_pb, n_ka, slots, row), BF16),
            pltpu.VMEM((ITERS, n_pb, n_ka, slots, row), BF16),
            pltpu.SemaphoreType.DMA,
            pltpu.SemaphoreType.DMA((ITERS,)),
            pltpu.SemaphoreType.DMA((ITERS,)),
            pltpu.SemaphoreType.DMA((2,)),
            pltpu.SemaphoreType.DMA((2,)),
        ],
        compiler_params=pltpu.CompilerParams(collective_id=0, has_side_effects=True),
    )(
        coupling[0, 0], jnp.transpose(phonon_occ[0], (2, 0, 1)), band_window[0, 0], pair_count[0], k_target[0], kq_source[0],
        velocity.reshape(directions * bands, width), lifetime,
    )
    return out.reshape(directions, bands, width)


def solution(mesh):
    placed = (
        P("pb", "ka", None, None, None),
        P("pb", "ka", None, None),
        P("pb", "ka", None, None),
        P("pb", "ka", None),
        P("pb", "ka", None),
        P("pb", "ka", None),
        P(None, None, "ka"),
        P(None, "ka"),
    )
    return jax.shard_map(
        functools.partial(shards, mesh.shape["pb"], mesh.shape["ka"]),
        mesh=mesh, in_specs=placed, out_specs=P(None, None, "ka"), check_vma=False,
    )
```

```python
import functools

import jax
import jax.numpy as jnp
from jax import lax
from jax.experimental import pallas as pl
from jax.experimental.pallas import tpu as pltpu
from jax.sharding import PartitionSpec as P

ITERS = 4
LANES = 128
UNROLLED = 16
F32 = jnp.float32
BF16 = jnp.bfloat16


def iota(shape, axis):
    return lax.broadcasted_iota(jnp.int32, shape, axis)


def mask(condition):
    return jnp.where(condition, 1.0, 0.0)


def dot(a, b, dims=((1,), (0,)), precision=None):
    return lax.dot_general(a, b, (dims, ((), ())), precision=precision, preferred_element_type=F32)


def column(row, wanted):
    rows, width = wanted.shape
    return jnp.sum(jnp.where(wanted, jnp.broadcast_to(row, (rows, width)), 0.0), axis=1, keepdims=True)


def each(count, act):
    if count <= 2 * UNROLLED:
        for distance in sorted(range(1, count), key=lambda d: -min(d, count - d)):
            act(distance)
    else:

        def body(distance, carry):
            act(distance)
            return carry

        lax.fori_loop(1, count, body, 0)


def kernel(
    n_pb, n_ka, directions,
    *refs,
):
    inputs, out_ref, held = refs[:8], refs[8], refs[9:17]
    weights, tables, send, recv, load_sem, send_sem, recv_sem, share_send, share_recv = refs[17:]
    coupling_ref, occ_ref, window_ref, count_ref, target_ref, source_ref, velocity_ref, lifetime_ref = held
    loads = [pltpu.make_async_copy(x, y, load_sem.at[i]) for i, (x, y) in enumerate(zip(inputs, held))]
    for load in loads:
        load.start()
    p, a = lax.axis_index("pb"), lax.axis_index("ka")
    me = p * n_ka + a
    devices = n_pb * n_ka
    tiles, bands = window_ref.shape
    slots = tiles // n_ka
    modes = occ_ref.shape[0]
    wide = bands * modes
    width = velocity_ref.shape[1]
    row = recv.shape[-1]
    used = directions * bands
    low = 256 // bands
    span = low * bands
    groups = tiles // low

    barrier = pltpu.get_barrier_semaphore()

    def peer(step):
        other = lax.rem(me + step, devices)
        return {"pb": other // n_ka, "ka": lax.rem(other, n_ka)}

    def greet(distance):
        pl.semaphore_signal(barrier, inc=1, device_id=peer(distance), device_id_type=pl.DeviceIdType.MESH)

    each(devices, greet)
    for load in loads[1:]:
        load.wait()

    eye = iota((tiles, tiles), 0) == iota((tiles, tiles), 1)
    owner = iota((tiles, n_ka), 0) // slots == iota((tiles, n_ka), 1)
    live = mask((iota((tiles, 1), 0) % slots).astype(F32) < column(count_ref[...].astype(F32), owner))
    source = column(source_ref[...].astype(F32), eye)
    target = column(target_ref[...].astype(F32), eye)
    target_lane = jnp.where(iota((tiles, row), 1) == used, target, 0.0)
    shown = window_ref[...].astype(F32) * live

    def tile_tables(shown, source):
        pick = mask(source == iota((tiles, width), 1).astype(F32)).astype(BF16)
        keep = jnp.concatenate([shown] * groups, axis=1)
        at = (tiles, groups * bands)
        keep = jnp.where(iota(at, 1) // bands == iota(at, 0) // low, keep, 0.0)
        return pick, jnp.concatenate([keep] * directions, axis=0)

    own = tile_tables(shown, source)
    tables[p] = jnp.concatenate(
        [shown, jnp.where(iota((tiles, LANES - bands), 1) == 0, source, 0.0)], axis=1
    ).astype(BF16)
    place = mask(
        (iota((tiles, directions * span), 1) % span) // bands == iota((tiles, directions * span), 0) % low
    )
    shape = (row, directions * span)
    spread = mask(
        ((iota(shape, 0) // bands) == (iota(shape, 1) // span)) & (iota(shape, 0) % bands == iota(shape, 1) % bands)
    ).astype(BF16)
    shape = (directions * groups * bands, row)
    fold = mask(
        ((iota(shape, 0) // (groups * bands)) == (iota(shape, 1) // bands))
        & (iota(shape, 0) % bands == iota(shape, 1) % bands)
    ).astype(BF16)

    pad = jnp.zeros((row - used, width), F32)
    velocity = jnp.concatenate([velocity_ref[...], pad], axis=0).T
    lifetime = jnp.concatenate([lifetime_ref[...]] * directions + [pad], axis=0).T

    shape = (modes, wide)
    occ = dot(
        occ_ref[:, 0, :], mask(iota(shape, 1) % modes == iota(shape, 0)), ((0,), (0,)), lax.Precision.HIGHEST
    )
    shape = (wide, LANES)
    start = (iota(shape, 1) % bands) * modes
    gather = mask((iota(shape, 0) >= start) & (iota(shape, 0) < start + modes)).astype(BF16)
    per = LANES // bands
    lane_block = iota((bands, LANES), 1) // bands
    loads[0].wait()
    weight = []
    for group in range(groups):
        halves = []
        for half in range(low // per):
            total = jnp.zeros((bands, LANES), F32)
            for inner in range(per):
                tile = group * low + half * per + inner
                value = coupling_ref[tile].astype(F32)
                value = (value * value * occ[tile : tile + 1, :]).astype(BF16)
                total = jnp.where(lane_block == inner, dot(value, gather), total)
            halves.append(total)
        weight.append(jnp.concatenate(halves, axis=1))
    weight = jnp.concatenate(weight, axis=0).astype(BF16)
    weights[p] = weight

    def share(distance, held, index):
        return pltpu.make_async_remote_copy(
            src_ref=held.at[p],
            dst_ref=held.at[p],
            send_sem=share_send.at[index],
            recv_sem=share_recv.at[index],
            device_id={"pb": lax.rem(p + distance, n_pb), "ka": a},
            device_id_type=pl.DeviceIdType.MESH,
        )

    def tile_terms(chosen, pick_keep_weight):
        keep, weight = pick_keep_weight
        chosen = (dot(chosen, spread) * place).astype(BF16)
        chosen = jnp.concatenate([chosen[:, i * span : (i + 1) * span] for i in range(directions)], axis=0)
        terms = (dot(chosen, weight, ((1,), (1,))) * keep).astype(BF16)
        terms = jnp.concatenate([terms[i * tiles : (i + 1) * tiles] for i in range(directions)], axis=1)
        return dot(terms, fold)

    deviation = lifetime * velocity

    terms = tile_terms(dot(own[0], deviation.astype(BF16)).astype(BF16), (own[1], weight)) + target_lane
    send[0, 0] = terms.astype(BF16).reshape(n_ka, slots, row)
    pl.semaphore_wait(barrier, devices - 1)

    def post_all(distance):
        to = peer(distance)
        pltpu.make_async_remote_copy(
            src_ref=send.at[0, 0, to["ka"]],
            dst_ref=recv.at[0, p, a],
            send_sem=send_sem.at[0],
            recv_sem=recv_sem.at[0],
            device_id=to,
            device_id_type=pl.DeviceIdType.MESH,
        ).start()

    each(devices, post_all)
    pltpu.make_async_copy(send.at[0, 0, a], recv.at[0, p, a], recv_sem.at[0]).start()
    for distance in range(1, n_pb):
        share(distance, tables, 0).start()
        share(distance, weights, 1).start()
    for index, held in enumerate((tables, weights)):
        part = held.at[pl.ds(0, n_pb - 1)]
        pltpu.make_async_copy(part, part, share_recv.at[index]).wait()
    picks, keeps = [], []
    for q in range(n_pb):
        table = tables[q].astype(F32)
        pick, keep = tile_tables(table[:, :bands], table[:, bands : bands + 1])
        picks.append(pick)
        keeps.append(keep)
    pick = jnp.concatenate(picks, axis=0)

    def receive(step):
        pltpu.make_async_copy(recv.at[step], recv.at[step], recv_sem.at[step]).wait()
        return recv[step].reshape(devices * slots, row)

    arrived = receive(0)
    shape = (devices * slots, width)
    scatter = mask(arrived[:, used : used + 1].astype(F32) == iota(shape, 1).astype(F32)).T.astype(BF16)
    deviation = lifetime * (velocity + dot(scatter, arrived))

    for step in range(1, ITERS):
        chosen = dot(pick, deviation.astype(BF16)).astype(BF16)
        for q in range(n_pb):
            terms = tile_terms(chosen[q * tiles : (q + 1) * tiles], (keeps[q], weights[q]))
            send[step, q] = terms.astype(BF16).reshape(n_ka, slots, row)

        def post(distance):
            other = lax.rem(a + distance, n_ka)
            pltpu.make_async_remote_copy(
                src_ref=send.at[step, :, other],
                dst_ref=recv.at[step, :, a],
                send_sem=send_sem.at[step],
                recv_sem=recv_sem.at[step],
                device_id={"pb": p, "ka": other},
                device_id_type=pl.DeviceIdType.MESH,
            ).start()

        each(n_ka, post)
        pltpu.make_async_copy(send.at[step, :, a], recv.at[step, :, a], recv_sem.at[step]).start()
        deviation = lifetime * (velocity + dot(scatter, receive(step)))
    out_ref[...] = deviation.T[:used]
    for step in range(ITERS):
        if step:
            pieces = [recv.at[step, :, pl.ds(0, n_ka - 1)]]
        else:
            pieces = [recv.at[0, pl.ds(0, n_pb - 1)]] if n_pb > 1 else []
            pieces = pieces + [recv.at[0, 0, pl.ds(0, n_ka - 1)]]
        for piece in pieces:
            pltpu.make_async_copy(piece, piece, send_sem.at[step]).wait()
    for index, held in enumerate((tables, weights)):
        part = held.at[pl.ds(0, n_pb - 1)]
        pltpu.make_async_copy(part, part, share_send.at[index]).wait()


def shards(n_pb, n_ka, coupling, phonon_occ, band_window, pair_count, k_target, kq_source, velocity, lifetime):
    tiles = coupling.shape[2]
    directions, bands, width = velocity.shape
    slots = tiles // n_ka
    low = 256 // bands
    row = -(-(directions * bands + 1) // LANES) * LANES
    vmem = pl.BlockSpec(memory_space=pltpu.VMEM)
    operands = (
        coupling[0, 0], jnp.transpose(phonon_occ[0], (2, 0, 1)), band_window[0, 0], pair_count[0], k_target[0],
        kq_source[0], velocity.reshape(directions * bands, width), lifetime,
    )
    out = pl.pallas_call(
        functools.partial(kernel, n_pb, n_ka, directions),
        out_shape=pltpu.VMEM((directions * bands, width), F32),
        in_specs=[pl.BlockSpec(memory_space=pl.ANY)] * len(operands),
        out_specs=vmem,
        scratch_shapes=[
            *[pltpu.VMEM(x.shape, x.dtype) for x in operands],
            pltpu.VMEM((n_pb, tiles // low * bands, low * bands), BF16),
            pltpu.VMEM((n_pb, tiles, LANES), BF16),
            pltpu.VMEM((ITERS, n_pb, n_ka, slots, row), BF16),
            pltpu.VMEM((ITERS, n_pb, n_ka, slots, row), BF16),
            pltpu.SemaphoreType.DMA((len(operands),)),
            pltpu.SemaphoreType.DMA((ITERS,)),
            pltpu.SemaphoreType.DMA((ITERS,)),
            pltpu.SemaphoreType.DMA((2,)),
            pltpu.SemaphoreType.DMA((2,)),
        ],
        compiler_params=pltpu.CompilerParams(collective_id=0, has_side_effects=True),
    )(*operands)
    return out.reshape(directions, bands, width)


def solution(mesh):
    placed = (
        P("pb", "ka", None, None, None),
        P("pb", "ka", None, None),
        P("pb", "ka", None, None),
        P("pb", "ka", None),
        P("pb", "ka", None),
        P("pb", "ka", None),
        P(None, None, "ka"),
        P(None, "ka"),
    )
    return jax.shard_map(
        functools.partial(shards, mesh.shape["pb"], mesh.shape["ka"]),
        mesh=mesh, in_specs=placed, out_specs=P(None, None, "ka"), check_vma=False,
    )
```
